32 devices in a mesh: node: 8 (over z, x), expert: 4 (over y, core).
Axes of the slice: x: 2, y: 2, z: 4, core: 2. Of those that a mesh axis runs over, the one named last changes fastest.
Arguments:
- tokens: bfloat16 [16384, 1024], P(('node', 'expert')), may hold values from -6 to 6
- queries: bfloat16 [16384, 1024], P(('node', 'expert')), may hold values from -6 to 6
- keys: bfloat16 [16384, 1024], P(('node', 'expert')), may hold values from -6 to 6
- values: bfloat16 [16384, 1024], P(('node', 'expert')), may hold values from -12 to 12
- neighbours: int32 [128, 8], P(('node', 'expert')), may hold values from 0 to 127, as said below
- live_bits: int32 [128, 8], P(('node', 'expert')), may hold values from 0 to 1, as said below
- out_proj: bfloat16 [1024, 1024], replicated, may hold values from -0.1875 to 0.1875
- norm_gain: float32 [1024], replicated, may hold values from 0.5 to 1.5
- router: bfloat16 [1024, 32], replicated, may hold values from -0.1875 to 0.1875
- expert: int32 [16384], P(('node', 'expert')), may hold values from 0 to 31, as said below
- slot: int32 [16384], P(('node', 'expert')), may hold values from 0 to 31, as said below
- w_up: bfloat16 [32, 1024, 4096], P(('node', 'expert')), may hold values from -0.1875 to 0.1875
- w_down: bfloat16 [32, 4096, 1024], P(('node', 'expert')), may hold values from -0.09375 to 0.09375
Outputs:
- layer_out: bfloat16 [16384, 1024], P(('node', 'expert'))
The draws below stay inside these ranges and needn't reach their ends.
Inputs may be any that keep to these rules, and one draw needn't show every extreme that they name: Tile g is held by device g // 4 in node-major order. neighbours[g, 0] is g itself; every listed tile is held by g's device or by the device one step before or after it along node with the same expert index (wrapping around); entry 1 is always one step before and entry 2 one step after. `live_bits`: entry 0 of every row is 1. Within the 512 tokens of one device, no two tokens share both expert and slot; some expert takes all 32 slots of every device. See expert: pairs (expert, slot) are distinct within one device's tokens.
All inputs are finite; a program needn't handle non-finite values.
Results may differ from the reference program's by a relative error of at most 0.0049.
Values may be sent and summed in bfloat16 or wider, within the bound.
No kernel may reach another device: no remote copies, remote signals or barrier semaphores. Data moves between devices by JAX's collectives and lax.ppermute only.
A program may use at most 192 MiB of HBM per device.

```python
import jax
import jax.numpy as jnp
from jax import lax

D = 1024
HEADS = 16
HEAD_DIM = 64
FF = 4096
TILE = 128
NB = 8
TOK_DEV = 512
EXPERTS = 32
CAP = 32
TOKENS = 16384
TILES = 128
N_NODE = 8
N_EXPERT = 4
DEVICES = 32


def query_key_pair(key):
    base_query = jnp.clip(jax.random.normal(jax.random.fold_in(key, 31), (TOKENS, D), jnp.float32) * 1.3, -6.0, 6.0)
    base_key = jnp.clip(jax.random.normal(jax.random.fold_in(key, 32), (TOKENS, D), jnp.float32) * 1.3, -6.0, 6.0)
    return (base_query, base_key)


def draw_queries(key, part):
    return query_key_pair(key)[0].astype(jnp.bfloat16)


def draw_keys(key, part):
    return query_key_pair(key)[1].astype(jnp.bfloat16)


def draw_neighbours(key, part):
    tile_count = TOKENS // TILE
    tiles_dev = TOK_DEV // TILE
    tile_ids = jnp.arange(tile_count, dtype=jnp.int32)
    device_of = tile_ids // tiles_dev
    node_of = device_of // N_EXPERT
    column_of = device_of % N_EXPERT
    steps = jax.random.randint(key, (tile_count, NB), -1, 2, jnp.int32)
    steps = steps.at[:, 0].set(0).at[:, 1].set(-1).at[:, 2].set(1)
    picks = jax.random.randint(jax.random.fold_in(key, 1), (tile_count, NB), 0, tiles_dev, jnp.int32)
    other_device = (node_of[:, None] + steps + N_NODE) % N_NODE * N_EXPERT + column_of[:, None]
    listed = other_device * tiles_dev + picks
    listed = listed.at[:, 0].set(tile_ids)
    return listed.astype(jnp.int32)


def draw_live_bits(key, part):
    tile_count = TOKENS // TILE
    drawn = jax.random.randint(jax.random.fold_in(key, 5), (tile_count, NB), 0, 4, jnp.int32)
    bits = jnp.where(drawn > 0, 1, 0).astype(jnp.int32)
    return bits.at[:, 0].set(1)


def route_cells(key):
    block_count = TOKENS // TOK_DEV
    cell_count = EXPERTS * CAP
    noise = jax.random.randint(jax.random.fold_in(key, 21), (block_count, cell_count), 0, 2 ** 18, jnp.int32)
    heat = jax.random.randint(jax.random.fold_in(key, 22), (EXPERTS,), 0, 2 ** 18, jnp.int32)
    hottest = jax.random.randint(jax.random.fold_in(key, 23), (), 0, EXPERTS, jnp.int32)
    owner_of = jnp.arange(cell_count, dtype=jnp.int32) // CAP
    scores = noise + heat[owner_of][None, :] + jnp.where(owner_of == hottest, 2 ** 19, 0)[None, :]
    ranked = jnp.argsort(-scores, axis=1, stable=True)[:, :TOK_DEV]
    return ranked.reshape(TOKENS).astype(jnp.int32)


def draw_expert(key, part):
    return (route_cells(key) // CAP).astype(jnp.int32)


def draw_slot(key, part):
    return (route_cells(key) % CAP).astype(jnp.int32)


def block_scale(key, extent, split, least, top_value):
    def one(position, parts):
        draws = jax.random.uniform(jax.random.fold_in(jax.random.fold_in(key, 6), position), (parts,), jnp.float32, least / len(split), top_value / len(split))
        return jnp.repeat(jnp.exp(draws), extent[position] // parts).reshape((-1,) + (1,) * (len(extent) - position - 1))

    loudness = one(*split[0])
    for cut in split[1:]:
        loudness = loudness * one(*cut)
    return loudness


def scatter_about(rng, extent, deviation, bound, pieces=(), held_as=jnp.bfloat16):
    values = jax.random.normal(rng, extent, jnp.float32) * deviation
    if len(pieces) > 0:
        values = block_scale(rng, extent, pieces, -0.22, 0.18) * values
    return jnp.clip(values, min=-bound, max=bound).astype(held_as)


def setup_inputs(seed: int = 0) -> dict:
    seeds = jax.random.split(jax.random.key(seed), 14)
    tokens = scatter_about(seeds[0], (TOKENS, D), 1.0, 6.0, ((0, 32),))
    queries = draw_queries(jax.random.fold_in(seeds[13], 71), 0)
    keys = draw_keys(jax.random.fold_in(seeds[13], 71), 0)
    values = scatter_about(seeds[3], (TOKENS, D), 2.0, 12.0, ((0, 32),))
    neighbours = draw_neighbours(jax.random.fold_in(seeds[13], 71), 0)
    live_bits = draw_live_bits(jax.random.fold_in(seeds[13], 71), 0)
    out_proj = scatter_about(seeds[6], (D, D), D ** -0.5, 0.1875)
    norm_gain = jnp.clip(1.0 + 0.1 * jax.random.normal(seeds[7], (D,), jnp.float32), 0.5, 1.5)
    router = scatter_about(seeds[8], (D, EXPERTS), D ** -0.5, 0.1875)
    expert = draw_expert(jax.random.fold_in(seeds[13], 71), 0)
    slot = draw_slot(jax.random.fold_in(seeds[13], 71), 0)
    w_up = scatter_about(seeds[11], (EXPERTS, D, FF), D ** -0.5, 0.1875, ((0, 32),))
    w_down = scatter_about(seeds[12], (EXPERTS, FF, D), FF ** -0.5, 0.09375, ((0, 32),))
    return dict(tokens=tokens, queries=queries, keys=keys, values=values, neighbours=neighbours, live_bits=live_bits, out_proj=out_proj, norm_gain=norm_gain, router=router, expert=expert, slot=slot, w_up=w_up, w_down=w_down)


score_scale = 0.125

def attend_tile(packed, key_tiles, value_tiles):
    query_tile, listed, bits = packed
    near_keys = key_tiles[listed].reshape(NB * TILE, HEADS, HEAD_DIM).astype(jnp.float32)
    near_values = value_tiles[listed].reshape(NB * TILE, HEADS, HEAD_DIM).astype(jnp.float32)
    query_heads = query_tile.reshape(TILE, HEADS, HEAD_DIM).astype(jnp.float32)
    scores = jnp.einsum('qhd,khd->hqk', query_heads, near_keys) * score_scale
    visible = jnp.repeat(bits, TILE) > 0
    masked = jnp.where(visible[None, None, :], scores, -jnp.inf)
    peak = lax.optimization_barrier(jnp.max(masked, axis=-1, keepdims=True))
    weights = jnp.exp(masked - peak)
    weights = (weights / lax.optimization_barrier(jnp.sum(weights, axis=-1, keepdims=True))).astype(jnp.bfloat16)
    mixed = jnp.einsum('hqk,khd->qhd', weights.astype(jnp.float32), near_values)
    return mixed.reshape(TILE, D).astype(jnp.bfloat16)

def reference(tokens, queries, keys, values, neighbours, live_bits, out_proj, norm_gain, router, expert, slot, w_up, w_down):
    key_tiles = keys.reshape(TILES, TILE, D)
    value_tiles = values.reshape(TILES, TILE, D)
    query_tiles = queries.reshape(TILES, TILE, D)
    attn = lax.map(lambda packed: attend_tile(packed, key_tiles, value_tiles), (query_tiles, neighbours, live_bits))
    attn = attn.reshape(TOKENS, D)
    hidden = tokens.astype(jnp.float32) + jnp.dot(attn, out_proj, preferred_element_type=jnp.float32)
    spread = lax.optimization_barrier(jnp.mean(hidden * hidden, axis=-1, keepdims=True))
    normed = (hidden * lax.rsqrt(spread + 1e-06) * norm_gain.astype(jnp.float32)[None, :]).astype(jnp.bfloat16)
    logits = jnp.dot(normed, router, preferred_element_type=jnp.float32)
    columns = jnp.arange(EXPERTS, dtype=jnp.int32)
    chosen = lax.optimization_barrier(jnp.sum(jnp.where(columns[None, :] == expert[:, None], logits, 0.0), axis=-1))
    gate = jax.nn.sigmoid(chosen)
    positions = jnp.arange(TOKENS, dtype=jnp.int32)
    target = expert * (DEVICES * CAP) + positions // TOK_DEV * CAP + slot
    table = jnp.full((EXPERTS * DEVICES * CAP,), TOKENS, jnp.int32).at[target].set(positions)
    padded = jnp.concatenate([normed, jnp.zeros((1, D), jnp.bfloat16)], axis=0)

    def run_expert(packed):
        index_rows, up_matrix, down_matrix = packed
        token_rows = padded[index_rows]
        lifted = jnp.dot(token_rows, up_matrix, preferred_element_type=jnp.float32)
        lifted = jax.nn.gelu(lifted, approximate=True).astype(jnp.bfloat16)
        return jnp.dot(lifted, down_matrix, preferred_element_type=jnp.float32).astype(jnp.bfloat16)
    results = lax.map(run_expert, (table.reshape(EXPERTS, DEVICES * CAP), w_up, w_down))
    expert_out = results.reshape(EXPERTS * DEVICES * CAP, D)[target]
    layer_out = hidden + gate[:, None] * expert_out.astype(jnp.float32)
    return layer_out.astype(jnp.bfloat16)
```

```python
import jax
import jax.numpy as jnp
from jax import lax
from jax.experimental import pallas as pl
from jax.experimental.pallas import tpu as pltpu
from jax.sharding import PartitionSpec as P


D = 1024
HEAD_DIM = 64
TILE = 128
NB = 8
PAIR = 2 * HEAD_DIM

score_scale = 0.125
SCALE2 = score_scale * 1.4426950408889634
CHUNK_PAIRS = (2, 2, 2, 2)


def attend_kernel(pos_ref, live_ref, q_ref, own_ref, near_ref, far_ref, o_ref, kv, sems):
    tiles = q_ref.shape[0] // TILE
    pairs = q_ref.shape[1] // PAIR
    nb = pos_ref.shape[1]
    copies = [
        pltpu.make_async_copy(ref, kv.at[pl.ds(2 * tiles * i, 2 * tiles)], sems.at[i])
        for i, ref in enumerate((own_ref, near_ref, far_ref))
    ]
    for copy in copies:
        copy.start()
    for copy in copies:
        copy.wait()
    first = lax.broadcasted_iota(jnp.int32, (TILE, PAIR), 1) < HEAD_DIM

    def unit(index):
        t = index // pairs
        p = index - t * pairs
        rows = pl.ds(pl.multiple_of(t * TILE, TILE), TILE)
        cols = pl.ds(pl.multiple_of(p * PAIR, PAIR), PAIR)
        q = q_ref[rows, cols]
        zero = jnp.zeros_like(q)
        two_heads = jnp.concatenate(
            [jnp.where(first, q, zero), jnp.where(first, zero, q)], axis=0
        )
        scores, biases, peak = [], [], None
        for j in range(nb):
            key = kv[pos_ref[t, j], :, cols]
            score = lax.dot_general(
                key, two_heads, (((1,), (1,)), ((), ())), preferred_element_type=jnp.float32
            )
            bias = jnp.where(live_ref[t, j] > 0, jnp.float32(0.0), jnp.float32(-jnp.inf))
            top = jnp.max(score, axis=0, keepdims=True) + bias
            peak = top if peak is None else jnp.maximum(peak, top)
            scores.append(score)
            biases.append(bias)
        base = peak * SCALE2
        total, out = None, None
        for j in range(0, nb, 2):
            powers = []
            for i in (j, j + 1):
                power = jnp.exp2(scores[i] * SCALE2 - (base - biases[i]))
                part = jnp.sum(power, axis=0, keepdims=True)
                total = part if total is None else total + part
                powers.append(power.astype(jnp.bfloat16))
            value = jnp.concatenate(
                [kv[pos_ref[t, i] + tiles, :, cols] for i in (j, j + 1)], axis=0
            )
            mixed = lax.dot_general(
                value,
                jnp.concatenate(powers, axis=0),
                (((0,), (0,)), ((), ())),
                preferred_element_type=jnp.float32,
            )
            out = mixed if out is None else out + mixed
        inverse = 1.0 / total
        both = jnp.concatenate(
            [
                out[:HEAD_DIM, :TILE] * inverse[:, :TILE],
                out[HEAD_DIM:, TILE:] * inverse[:, TILE:],
            ],
            axis=0,
        )
        o_ref[rows, cols] = both.T.astype(jnp.bfloat16)

    def step(i, carry):
        unit(2 * i)
        unit(2 * i + 1)
        return carry

    lax.fori_loop(0, tiles * pairs // 2, step, 0)


def attend(queries, first_col, blocks, position, live_bits):
    tok, width = queries.shape[0], blocks[0].shape[1]
    tiles = tok // TILE
    blocks = [block.reshape(2 * tiles, TILE, width) for block in blocks]
    query = lax.slice_in_dim(queries, first_col, first_col + width, axis=1)
    return pl.pallas_call(
        attend_kernel,
        out_shape=jax.ShapeDtypeStruct((tok, width), jnp.bfloat16),
        grid_spec=pltpu.PrefetchScalarGridSpec(
            num_scalar_prefetch=2,
            grid=(1,),
            in_specs=[pl.BlockSpec((tok, width), lambda i, *_: (0, 0))]
            + [pl.BlockSpec(memory_space=pl.ANY)] * 3,
            out_specs=pl.BlockSpec((tok, width), lambda i, *_: (0, 0)),
            scratch_shapes=[
                pltpu.VMEM((6 * tiles, TILE, width), jnp.bfloat16),
                pltpu.SemaphoreType.DMA((3,)),
            ],
        ),
        compiler_params=pltpu.CompilerParams(vmem_limit_bytes=40 << 20),
        cost_estimate=pl.CostEstimate(
            flops=4 * tok * NB * TILE * width * 2,
            transcendentals=tok * NB * TILE * width // HEAD_DIM,
            bytes_accessed=8 * tok * width * 2,
        ),
        name="attend",
    )(position, live_bits, query, *blocks)


def layer(
    tokens,
    queries,
    keys,
    values,
    neighbours,
    live_bits,
    out_proj,
    norm_gain,
    router,
    expert,
    slot,
    w_up,
    w_down,
):
    tok_dev = tokens.shape[0]
    tiles_dev = tok_dev // TILE
    experts = router.shape[1]
    cap = 2 * tok_dev // experts
    my_node = lax.axis_index("node")
    node_count = lax.axis_size("node")
    column_count = lax.axis_size("expert")
    swap = [(i, i ^ 1) for i in range(node_count)]
    onward = [(i, (i + 2 - 4 * (i % 2)) % node_count) for i in range(node_count)]
    is_odd = my_node % 2
    owner_node = neighbours // tiles_dev // column_count
    offset = (owner_node - my_node + node_count) % node_count
    near_offset = jnp.where(is_odd == 1, node_count - 1, 1)
    block_of = jnp.where(offset == 0, 0, jnp.where(offset == near_offset, 1, 2))
    position = block_of * (2 * tiles_dev) + neighbours % tiles_dev
    mixed = []
    col = 0
    for pairs in CHUNK_PAIRS:
        width = pairs * PAIR
        own = jnp.concatenate([keys[:, col : col + width], values[:, col : col + width]], axis=0)
        near = lax.ppermute(own, "node", swap)
        far = lax.ppermute(near, "node", onward)
        mixed.append(attend(queries, col, (own, near, far), position, live_bits))
        col += width
    attn = jnp.concatenate(mixed, axis=1)
    hidden = tokens.astype(jnp.float32) + jnp.dot(
        attn, out_proj, preferred_element_type=jnp.float32
    )
    spread = jnp.mean(hidden * hidden, axis=-1, keepdims=True)
    normed = (hidden * lax.rsqrt(spread + 1e-06) * norm_gain[None, :]).astype(jnp.bfloat16)
    logits = jnp.dot(normed, router, preferred_element_type=jnp.float32)
    columns = lax.iota(jnp.int32, experts)
    chosen = jnp.sum(jnp.where(columns[None, :] == expert[:, None], logits, 0.0), axis=-1)
    gate = jax.nn.sigmoid(chosen)
    slot_cell = expert * cap + slot
    one_hot = (lax.iota(jnp.int32, experts * cap)[:, None] == slot_cell[None, :]).astype(
        jnp.bfloat16
    )
    outgoing = jnp.dot(one_hot, normed, preferred_element_type=jnp.float32).astype(jnp.bfloat16)
    up_matrix = w_up[0]
    down_matrix = w_down[0]
    block = lax.all_to_all(
        outgoing.reshape(experts, 1, cap, D),
        ("node", "expert"),
        split_axis=0,
        concat_axis=1,
        tiled=True,
    )
    token_rows = block.reshape(-1, D)
    lifted = jnp.dot(token_rows, up_matrix, preferred_element_type=jnp.float32)
    lifted = jax.nn.gelu(lifted, approximate=True).astype(jnp.bfloat16)
    result = jnp.dot(lifted, down_matrix, preferred_element_type=jnp.float32).astype(jnp.bfloat16)
    returned = lax.all_to_all(
        result.reshape(block.shape), ("node", "expert"), split_axis=1, concat_axis=0, tiled=True
    )
    flat_back = returned.reshape(experts * cap, D)
    expert_out = jnp.einsum("ct,cd->td", one_hot, flat_back, preferred_element_type=jnp.float32)
    layer_out = hidden + gate[:, None] * expert_out
    return layer_out.astype(jnp.bfloat16)


def solution(mesh):
    in_specs = (
        P(("node", "expert"), None),
        P(("node", "expert"), None),
        P(("node", "expert"), None),
        P(("node", "expert"), None),
        P(("node", "expert"), None),
        P(("node", "expert"), None),
        P(),
        P(),
        P(),
        P(("node", "expert")),
        P(("node", "expert")),
        P(("node", "expert"), None, None),
        P(("node", "expert"), None, None),
    )
    out_specs = P(("node", "expert"), None)
    return jax.shard_map(layer, mesh=mesh, in_specs=in_specs, out_specs=out_specs, check_vma=False)
```

```python
import jax
import jax.numpy as jnp
from jax import lax
from jax.experimental import pallas as pl
from jax.experimental.pallas import tpu as pltpu
from jax.sharding import PartitionSpec as P


D = 1024
HEAD_DIM = 64
TILE = 128
NB = 8
PAIR = 2 * HEAD_DIM

score_scale = 0.125
SCALE2 = score_scale * 1.4426950408889634
SEND_PAIRS = (1, 1, 1, 1, 1, 1, 1, 1)
GROUPS = (1, 1, 1, 1, 1, 1, 1, 1)
PARTS = 2
EARLY = 6
SPLIT = 4
SIDE = 128


def pack_kernel(cols, keys_ref, values_ref, *outs):
    tok = keys_ref.shape[0]
    for (col, width), out in zip(cols, outs):
        out[:tok] = keys_ref[:, col : col + width]
        out[tok:] = values_ref[:, col : col + width]


def pack(keys, values, cols):
    tok, span = keys.shape[0], cols[-1][0] + cols[-1][1]
    return pl.pallas_call(
        lambda *refs: pack_kernel(cols, *refs),
        out_shape=[jax.ShapeDtypeStruct((2 * tok, width), keys.dtype) for _, width in cols],
        grid=(1,),
        in_specs=[pl.BlockSpec((tok, span), lambda i: (0, 0))] * 2,
        out_specs=[pl.BlockSpec((2 * tok, width), lambda i: (0, 0)) for _, width in cols],
        name="pack",
    )(keys, values)


def attend_kernel(sizes, *refs):
    pos_ref, live_ref, q_ref = refs[:3]
    blocks = refs[3 : 3 + 3 * len(sizes)]
    o_ref, kv, score_even, score_odd, peak_even, peak_odd, sems = refs[3 + 3 * len(sizes) :]
    tiles = q_ref.shape[0] // TILE
    pairs = q_ref.shape[1] // PAIR
    nb = pos_ref.shape[1]
    copies, col = [], 0
    for i, size in enumerate(sizes):
        for j in range(3):
            target = kv.at[pl.ds(2 * tiles * j, 2 * tiles), :, pl.ds(col, size * PAIR)]
            copies.append(pltpu.make_async_copy(blocks[3 * i + j], target, sems.at[3 * i + j]))
        col += size * PAIR
    for copy in copies:
        copy.start()
    for copy in copies:
        copy.wait()
    first = lax.broadcasted_iota(jnp.int32, (TILE, PAIR), 1) < HEAD_DIM
    ones = jnp.ones((16, 2 * TILE), jnp.bfloat16)
    count = tiles * pairs

    def place(index):
        t = index // pairs
        p = index - t * pairs
        return (
            t,
            pl.ds(pl.multiple_of(t * TILE, TILE), TILE),
            pl.ds(pl.multiple_of(p * PAIR, PAIR), PAIR),
        )

    def bias(t, j):
        return jnp.where(live_ref[t, j] > 0, jnp.float32(0.0), jnp.float32(-jnp.inf))

    def score(index, score_ref, peak_ref):
        t, rows, cols = place(index)
        q = q_ref[rows, cols]
        zero = jnp.zeros_like(q)
        two_heads = jnp.concatenate(
            [jnp.where(first, q, zero), jnp.where(first, zero, q)], axis=0
        )
        peak = None
        for j in range(nb):
            part = lax.dot_general(
                kv[pos_ref[t, j], :, cols],
                two_heads,
                (((1,), (1,)), ((), ())),
                preferred_element_type=jnp.float32,
            )
            score_ref[pl.ds(j * TILE, TILE), :] = part
            top = jnp.max(part.reshape(TILE // 8, 8, 2 * TILE), axis=0) + bias(t, j)
            peak = top if peak is None else jnp.maximum(peak, top)
        peak_ref[...] = peak

    def mix(index, score_ref, peak_ref):
        t, rows, cols = place(index)
        base = jnp.max(peak_ref[...], axis=0, keepdims=True) * SCALE2
        out = None
        for j in range(0, nb, 2):
            powers = [
                jnp.exp2(
                    score_ref[pl.ds(i * TILE, TILE), :] * SCALE2 - (base - bias(t, i))
                ).astype(jnp.bfloat16)
                for i in (j, j + 1)
            ]
            value = jnp.concatenate(
                [kv[pos_ref[t, i] + tiles, :, cols] for i in (j, j + 1)], axis=0
            )
            part = jnp.dot(
                jnp.concatenate([value.T, ones], axis=0),
                jnp.concatenate(powers, axis=0),
                preferred_element_type=jnp.float32,
            )
            out = part if out is None else out + part
        inverse = 1.0 / out[PAIR : PAIR + 1]
        both = jnp.concatenate(
            [
                out[:HEAD_DIM, :TILE] * inverse[:, :TILE],
                out[HEAD_DIM:PAIR, TILE:] * inverse[:, TILE:],
            ],
            axis=0,
        )
        o_ref[rows, cols] = both.T.astype(jnp.bfloat16)

    score(0, score_even, peak_even)

    def step(i, carry):
        score(2 * i + 1, score_odd, peak_odd)
        mix(2 * i, score_even, peak_even)
        score(jnp.minimum(2 * i + 2, count - 1), score_even, peak_even)
        mix(2 * i + 1, score_odd, peak_odd)
        return carry

    lax.fori_loop(0, count // 2, step, 0)


def attend(queries, col, sizes, blocks, position, live_bits):
    tok, width = queries.shape[0], sum(sizes) * PAIR
    if col % width:
        queries, col = lax.slice_in_dim(queries, col, col + width, axis=1), 0
    column = col // width
    tiles, nb = tok // TILE, position.shape[1]
    blocks = [block.reshape(2 * tiles, TILE, block.shape[1]) for block in blocks]
    return pl.pallas_call(
        lambda *refs: attend_kernel(sizes, *refs),
        out_shape=jax.ShapeDtypeStruct((tok, width), jnp.bfloat16),
        grid_spec=pltpu.PrefetchScalarGridSpec(
            num_scalar_prefetch=2,
            grid=(1,),
            in_specs=[pl.BlockSpec((tok, width), lambda i, *_: (0, column))]
            + [pl.BlockSpec(memory_space=pl.ANY)] * len(blocks),
            out_specs=pl.BlockSpec((tok, width), lambda i, *_: (0, 0)),
            scratch_shapes=[
                pltpu.VMEM((6 * tiles, TILE, width), jnp.bfloat16),
                pltpu.VMEM((nb * TILE, 2 * TILE), jnp.float32),
                pltpu.VMEM((nb * TILE, 2 * TILE), jnp.float32),
                pltpu.VMEM((8, 2 * TILE), jnp.float32),
                pltpu.VMEM((8, 2 * TILE), jnp.float32),
                pltpu.SemaphoreType.DMA((len(blocks),)),
            ],
        ),
        compiler_params=pltpu.CompilerParams(vmem_limit_bytes=24 << 20),
        cost_estimate=pl.CostEstimate(
            flops=4 * tok * NB * TILE * width * 2,
            transcendentals=tok * NB * TILE * width // HEAD_DIM,
            bytes_accessed=8 * tok * width * 2,
        ),
        name="attend",
    )(position, live_bits, queries, *blocks)


def norm_kernel(pre_ref, *refs):
    attn_refs, refs = refs[:-9], refs[-9:]
    w_ref, gain_ref, cell_ref, hidden_ref, normed_ref, out_ref, kept, staged, sems = refs
    attn = jnp.concatenate([ref[...] for ref in attn_refs], axis=1)
    hidden = pre_ref[...] + jnp.dot(attn, w_ref[...], preferred_element_type=jnp.float32)
    kept[...] = hidden
    copies = [pltpu.make_async_copy(kept, hidden_ref, sems.at[SPLIT])]
    copies[0].start()
    spread = jnp.mean(hidden * hidden, axis=-1, keepdims=True)
    normed = (hidden * lax.rsqrt(spread + 1e-06) * gain_ref[...]).astype(jnp.bfloat16)
    normed_ref[...] = normed
    step = staged.shape[0] // SPLIT
    for i in range(SPLIT):
        cells = lax.broadcasted_iota(jnp.int32, (step, cell_ref.shape[1]), 0) + i * step
        one_hot = (cells == cell_ref[...]).astype(jnp.bfloat16)
        staged[pl.ds(i * step, step)] = jnp.dot(
            one_hot, normed, preferred_element_type=jnp.float32
        ).astype(jnp.bfloat16)
        rows = pl.ds(i * step, step)
        copies.append(pltpu.make_async_copy(staged.at[rows], out_ref.at[rows], sems.at[i]))
        copies[-1].start()
    for copy in copies:
        copy.wait()


def norm_and_send(pre, attn, weights, depth, gain, cell, cells):
    tok, width = pre.shape
    rest = weights.shape[0] - depth
    if depth % rest:
        weights, depth = weights[depth:], 0
    whole = pl.BlockSpec(memory_space=pltpu.VMEM)
    return pl.pallas_call(
        norm_kernel,
        out_shape=[
            pltpu.HBM((tok, width), jnp.float32),
            jax.ShapeDtypeStruct((tok, width), jnp.bfloat16),
            pltpu.HBM((cells, width), jnp.bfloat16),
        ],
        grid=(1,),
        in_specs=[whole] * (1 + len(attn))
        + [pl.BlockSpec((rest, width), lambda i: (depth // rest, 0)), whole, whole],
        out_specs=[
            pl.BlockSpec(memory_space=pltpu.HBM),
            whole,
            pl.BlockSpec(memory_space=pltpu.HBM),
        ],
        scratch_shapes=[
            pltpu.VMEM((tok, width), jnp.float32),
            pltpu.VMEM((cells, width), jnp.bfloat16),
            pltpu.SemaphoreType.DMA((SPLIT + 1,)),
        ],
        compiler_params=pltpu.CompilerParams(vmem_limit_bytes=24 << 20),
        name="norm",
    )(pre, *attn, weights, gain[None, :], cell[None, :])


def chosen_rows(cell, back):
    cells = lax.broadcasted_iota(jnp.int32, (cell.shape[0], back.shape[0]), 1)
    one_hot = (cells == cell).astype(jnp.bfloat16)
    return jnp.dot(one_hot, back, preferred_element_type=jnp.float32)


def rows_kernel(hidden_ref, gate_ref, cell_ref, next_ref, back_ref, out_ref):
    width = hidden_ref.shape[1]
    rows = chosen_rows(cell_ref[...], back_ref[...])
    out_ref[:, :width] = hidden_ref[...] + gate_ref[...] * rows
    lane = lax.broadcasted_iota(jnp.int32, (out_ref.shape[0], SIDE), 1)
    out_ref[:, width:] = jnp.where(
        lane == 0, gate_ref[...], next_ref[...].astype(jnp.float32)
    )


def first_rows(hidden, gate, cell, next_cell, back):
    tok, width = hidden.shape
    return pl.pallas_call(
        rows_kernel,
        out_shape=jax.ShapeDtypeStruct((tok, width + SIDE), jnp.float32),
        compiler_params=pltpu.CompilerParams(vmem_limit_bytes=24 << 20),
        name="rows",
    )(hidden, gate, cell[:, None], next_cell[:, None], back)


def final_kernel(base_ref, back, out_ref, staged, sems):
    tok, width = staged.shape
    step = tok // SPLIT
    copies = []
    for i in range(SPLIT):
        rows = pl.ds(i * step, step)
        gate = base_ref[rows, width : width + 1]
        cell = base_ref[rows, width + 1 : width + 2].astype(jnp.int32)
        chosen = chosen_rows(cell, back[...])
        staged[rows] = (base_ref[rows, :width] + gate * chosen).astype(jnp.bfloat16)
        copies.append(pltpu.make_async_copy(staged.at[rows], out_ref.at[rows], sems.at[i]))
        copies[-1].start()
    for copy in copies:
        copy.wait()


def last_rows(base, back):
    shape = (base.shape[0], base.shape[1] - SIDE)
    return pl.pallas_call(
        final_kernel,
        out_shape=pltpu.HBM(shape, jnp.bfloat16),
        in_specs=[pl.BlockSpec(memory_space=pltpu.VMEM)] * 2,
        out_specs=pl.BlockSpec(memory_space=pltpu.HBM),
        scratch_shapes=[
            pltpu.VMEM(shape, jnp.bfloat16),
            pltpu.SemaphoreType.DMA((SPLIT,)),
        ],
        compiler_params=pltpu.CompilerParams(vmem_limit_bytes=16 << 20),
        name="final",
    )(base, back)


def expert_kernel(x_ref, up_ref, down_ref, o_ref, total):
    i = pl.program_id(0)
    last = pl.num_programs(0) - 1
    half = up_ref.shape[1] // 2
    part = None
    for s in range(2):
        lifted = jnp.dot(
            x_ref[...], up_ref[:, s * half : (s + 1) * half], preferred_element_type=jnp.float32
        )
        lifted = jax.nn.gelu(lifted, approximate=True).astype(jnp.bfloat16)
        down = jnp.dot(
            lifted, down_ref[s * half : (s + 1) * half, :], preferred_element_type=jnp.float32
        )
        part = down if part is None else part + down

    @pl.when(i == 0)
    def _():
        total[...] = part

    @pl.when(jnp.logical_and(i > 0, i < last))
    def _():
        total[...] += part

    @pl.when(i == last)
    def _():
        o_ref[...] = (total[...] + part).astype(jnp.bfloat16)


def run_expert(rows, up_matrix, down_matrix):
    count, hidden = rows.shape[0], up_matrix.shape[1]
    step = 1024
    return pl.pallas_call(
        expert_kernel,
        out_shape=jax.ShapeDtypeStruct((count, D), jnp.bfloat16),
        grid=(hidden // step,),
        in_specs=[
            pl.BlockSpec((count, D), lambda i: (0, 0)),
            pl.BlockSpec((D, step), lambda i: (0, i)),
            pl.BlockSpec((step, D), lambda i: (i, 0)),
        ],
        out_specs=pl.BlockSpec((count, D), lambda i: (0, 0)),
        scratch_shapes=[pltpu.VMEM((count, D), jnp.float32)],
        compiler_params=pltpu.CompilerParams(vmem_limit_bytes=58 << 20),
        cost_estimate=pl.CostEstimate(
            flops=4 * count * D * hidden, transcendentals=count * hidden, bytes_accessed=4 * D * hidden
        ),
        name="expert",
    )(rows, up_matrix, down_matrix)


def layer(
    tokens,
    queries,
    keys,
    values,
    neighbours,
    live_bits,
    out_proj,
    norm_gain,
    router,
    expert,
    slot,
    w_up,
    w_down,
):
    tok_dev = tokens.shape[0]
    tiles_dev = tok_dev // TILE
    experts = router.shape[1]
    cap = 2 * tok_dev // experts
    my_node = lax.axis_index("node")
    node_count = lax.axis_size("node")
    column_count = lax.axis_size("expert")
    swap = [(i, i ^ 1) for i in range(node_count)]
    onward = [(i, (i + 2 - 4 * (i % 2)) % node_count) for i in range(node_count)]
    is_odd = my_node % 2
    owner_node = neighbours // tiles_dev // column_count
    offset = (owner_node - my_node + node_count) % node_count
    near_offset = jnp.where(is_odd == 1, node_count - 1, 1)
    block_of = jnp.where(offset == 0, 0, jnp.where(offset == near_offset, 1, 2))
    position = block_of * (2 * tiles_dev) + neighbours % tiles_dev
    cols, col = [], 0
    for pairs in SEND_PAIRS:
        cols.append((col, pairs * PAIR))
        col += pairs * PAIR
    owns = pack(keys, values, cols[:1])
    owns += pack(keys, values, cols[1:])
    sent = []
    for i, own in enumerate(owns):
        near = lax.ppermute(own, "node", swap)
        far = lax.ppermute(near, "node", onward)
        sent.append((own, near, far))
    mixed, i, col = [], 0, 0
    for length in GROUPS:
        sizes = SEND_PAIRS[i : i + length]
        width = sum(sizes) * PAIR
        blocks = [block for chunk in sent[i : i + length] for block in chunk]
        mixed.append(attend(queries, col, sizes, blocks, position, live_bits))
        i, col = i + length, col + width
    part_cap = cap // PARTS
    slot_cell = expert * part_cap + slot % part_cap
    cells = [jnp.where(slot // part_cap == part, slot_cell, -1) for part in range(PARTS)]
    early = jnp.concatenate(mixed[:EARLY], axis=1)
    depth = early.shape[1]
    pre = tokens.astype(jnp.float32) + jnp.dot(
        early, out_proj[:depth], preferred_element_type=jnp.float32
    )
    hidden, normed, outgoing = norm_and_send(
        pre, mixed[EARLY:], out_proj, depth, norm_gain, cells[0], experts * part_cap
    )
    logits = jnp.dot(normed, router, preferred_element_type=jnp.float32)
    columns = lax.iota(jnp.int32, experts)
    chosen = jnp.sum(jnp.where(columns[None, :] == expert[:, None], logits, 0.0), axis=-1)
    gate = jax.nn.sigmoid(chosen)[:, None]
    layer_out = hidden
    for part in range(PARTS):
        if part:
            one_hot = lax.iota(jnp.int32, experts * part_cap)[:, None] == cells[part][None, :]
            outgoing = jnp.dot(
                one_hot.astype(jnp.bfloat16), normed, preferred_element_type=jnp.float32
            ).astype(jnp.bfloat16)
        block = lax.all_to_all(
            outgoing.reshape(experts, part_cap, D),
            ("node", "expert"),
            split_axis=0,
            concat_axis=0,
            tiled=True,
        )
        result = run_expert(block.reshape(-1, D), w_up[0], w_down[0])
        returned = lax.all_to_all(
            result.reshape(block.shape),
            ("node", "expert"),
            split_axis=0,
            concat_axis=0,
            tiled=True,
        )
        returned = returned.reshape(experts * part_cap, D)
        if part < PARTS - 1:
            layer_out = first_rows(layer_out, gate, cells[part], cells[part + 1], returned)
        else:
            layer_out = last_rows(layer_out, returned)
    return layer_out


def solution(mesh):
    in_specs = (
        P(("node", "expert"), None),
        P(("node", "expert"), None),
        P(("node", "expert"), None),
        P(("node", "expert"), None),
        P(("node", "expert"), None),
        P(("node", "expert"), None),
        P(),
        P(),
        P(),
        P(("node", "expert")),
        P(("node", "expert")),
        P(("node", "expert"), None, None),
        P(("node", "expert"), None, None),
    )
    out_specs = P(("node", "expert"), None)
    return jax.shard_map(layer, mesh=mesh, in_specs=in_specs, out_specs=out_specs, check_vma=False)
```

```python
import jax
import jax.numpy as jnp
from jax import lax
from jax.experimental import pallas as pl
from jax.experimental.pallas import tpu as pltpu
from jax.sharding import PartitionSpec as P


D = 1024
HEAD_DIM = 64
TILE = 128
NB = 8
PAIR = 2 * HEAD_DIM

score_scale = 0.125
SCALE2 = score_scale * 1.4426950408889634
SEND_PAIRS = (1, 1, 1, 1, 1, 1, 1, 1)
GROUPS = (1, 1, 1, 1, 1, 1, 1, 1)
PARTS = 2
EARLY = 7
SPLIT = 4
UNROLLED = 4
SIDE = 128


def pack_kernel(cols, keys_ref, values_ref, *outs):
    tok = keys_ref.shape[0]
    for (col, width), out in zip(cols, outs):
        out[:tok] = keys_ref[:, col : col + width]
        out[tok:] = values_ref[:, col : col + width]


def pack(keys, values, cols):
    tok, span = keys.shape[0], cols[-1][0] + cols[-1][1]
    return pl.pallas_call(
        lambda *refs: pack_kernel(cols, *refs),
        out_shape=[jax.ShapeDtypeStruct((2 * tok, width), keys.dtype) for _, width in cols],
        grid=(1,),
        in_specs=[pl.BlockSpec((tok, span), lambda i: (0, 0))] * 2,
        out_specs=[pl.BlockSpec((2 * tok, width), lambda i: (0, 0)) for _, width in cols],
        name="pack",
    )(keys, values)


def attend_kernel(sizes, *refs):
    pos_ref, live_ref, q_ref = refs[:3]
    blocks = refs[3 : 3 + 3 * len(sizes)]
    o_ref, kv, score_even, score_odd, peak_even, peak_odd, sems = refs[3 + 3 * len(sizes) :]
    tiles = q_ref.shape[0] // TILE
    pairs = q_ref.shape[1] // PAIR
    nb = pos_ref.shape[1]
    copies, col = [], 0
    for i, size in enumerate(sizes):
        for j in range(3):
            target = kv.at[pl.ds(2 * tiles * j, 2 * tiles), :, pl.ds(col, size * PAIR)]
            copies.append(pltpu.make_async_copy(blocks[3 * i + j], target, sems.at[3 * i + j]))
        col += size * PAIR
    for copy in copies:
        copy.start()
    for copy in copies:
        copy.wait()
    first = lax.broadcasted_iota(jnp.int32, (TILE, PAIR), 1) < HEAD_DIM
    ones = jnp.ones((16, 2 * TILE), jnp.bfloat16)
    count = tiles * pairs

    def place(index):
        t = index // pairs
        p = index - t * pairs
        if isinstance(index, int):
            return t, pl.ds(t * TILE, TILE), pl.ds(p * PAIR, PAIR)
        return (
            t,
            pl.ds(pl.multiple_of(t * TILE, TILE), TILE),
            pl.ds(pl.multiple_of(p * PAIR, PAIR), PAIR),
        )

    def bias(t, j):
        return jnp.where(live_ref[t, j] > 0, jnp.float32(0.0), jnp.float32(-jnp.inf))

    def score(index, score_ref, peak_ref):
        t, rows, cols = place(index)
        q = q_ref[rows, cols]
        zero = jnp.zeros_like(q)
        two_heads = jnp.concatenate(
            [jnp.where(first, q, zero), jnp.where(first, zero, q)], axis=0
        )
        peak = None
        for j in range(nb):
            part = lax.dot_general(
                kv[pos_ref[t, j], :, cols],
                two_heads,
                (((1,), (1,)), ((), ())),
                preferred_element_type=jnp.float32,
            )
            score_ref[pl.ds(j * TILE, TILE), :] = part
            top = jnp.max(part.reshape(TILE // 8, 8, 2 * TILE), axis=0) + bias(t, j)
            peak = top if peak is None else jnp.maximum(peak, top)
        peak_ref[...] = peak

    def mix(index, score_ref, peak_ref):
        t, rows, cols = place(index)
        base = jnp.max(peak_ref[...], axis=0, keepdims=True) * SCALE2
        out = None
        for j in range(0, nb, 2):
            powers = [
                jnp.exp2(
                    score_ref[pl.ds(i * TILE, TILE), :] * SCALE2 - (base - bias(t, i))
                ).astype(jnp.bfloat16)
                for i in (j, j + 1)
            ]
            value = jnp.concatenate(
                [kv[pos_ref[t, i] + tiles, :, cols] for i in (j, j + 1)], axis=0
            )
            part = jnp.dot(
                jnp.concatenate([value.T, ones], axis=0),
                jnp.concatenate(powers, axis=0),
                preferred_element_type=jnp.float32,
            )
            out = part if out is None else out + part
        inverse = 1.0 / out[PAIR : PAIR + 1]
        both = jnp.concatenate(
            [
                out[:HEAD_DIM, :TILE] * inverse[:, :TILE],
                out[HEAD_DIM:PAIR, TILE:] * inverse[:, TILE:],
            ],
            axis=0,
        )
        o_ref[rows, cols] = both.T.astype(jnp.bfloat16)

    slots = ((score_even, peak_even), (score_odd, peak_odd))
    score(0, *slots[0])
    if count <= UNROLLED:
        for index in range(count):
            if index + 1 < count:
                score(index + 1, *slots[(index + 1) % 2])
            mix(index, *slots[index % 2])
        return

    def step(i, carry):
        for half in range(2):
            index = 2 * i + half
            score(jnp.minimum(index + 1, count - 1), *slots[1 - half])
            mix(index, *slots[half])
        return carry

    lax.fori_loop(0, count // 2, step, 0)


def attend(queries, col, sizes, blocks, position, live_bits):
    tok, width = queries.shape[0], sum(sizes) * PAIR
    if col % width:
        queries, col = lax.slice_in_dim(queries, col, col + width, axis=1), 0
    column = col // width
    tiles, nb = tok // TILE, position.shape[1]
    blocks = [block.reshape(2 * tiles, TILE, block.shape[1]) for block in blocks]
    return pl.pallas_call(
        lambda *refs: attend_kernel(sizes, *refs),
        out_shape=jax.ShapeDtypeStruct((tok, width), jnp.bfloat16),
        grid_spec=pltpu.PrefetchScalarGridSpec(
            num_scalar_prefetch=2,
            grid=(1,),
            in_specs=[pl.BlockSpec((tok, width), lambda i, *_: (0, column))]
            + [pl.BlockSpec(memory_space=pl.ANY)] * len(blocks),
            out_specs=pl.BlockSpec((tok, width), lambda i, *_: (0, 0)),
            scratch_shapes=[
                pltpu.VMEM((6 * tiles, TILE, width), jnp.bfloat16),
                pltpu.VMEM((nb * TILE, 2 * TILE), jnp.float32),
                pltpu.VMEM((nb * TILE, 2 * TILE), jnp.float32),
                pltpu.VMEM((8, 2 * TILE), jnp.float32),
                pltpu.VMEM((8, 2 * TILE), jnp.float32),
                pltpu.SemaphoreType.DMA((len(blocks),)),
            ],
        ),
        compiler_params=pltpu.CompilerParams(vmem_limit_bytes=24 << 20),
        cost_estimate=pl.CostEstimate(
            flops=4 * tok * NB * TILE * width * 2,
            transcendentals=tok * NB * TILE * width // HEAD_DIM,
            bytes_accessed=8 * tok * width * 2,
        ),
        name="attend",
    )(position, live_bits, queries, *blocks)


def norm_kernel(pre_ref, *refs):
    attn_refs, refs = refs[:-9], refs[-9:]
    w_ref, gain_ref, cell_ref, hidden_ref, normed_ref, out_ref, kept, staged, sems = refs
    copies = []
    step = pre_ref.shape[0] // SPLIT
    for i in range(SPLIT):
        rows = pl.ds(i * step, step)
        attn = jnp.concatenate([ref[rows] for ref in attn_refs], axis=1)
        hidden = pre_ref[rows] + jnp.dot(
            attn, w_ref[...], preferred_element_type=jnp.float32
        )
        kept[rows] = hidden
        copies.append(
            pltpu.make_async_copy(kept.at[rows], hidden_ref.at[rows], sems.at[SPLIT + i])
        )
        copies[-1].start()
        spread = jnp.mean(hidden * hidden, axis=-1, keepdims=True)
        normed_ref[rows] = (hidden * lax.rsqrt(spread + 1e-06) * gain_ref[...]).astype(
            jnp.bfloat16
        )
    normed = normed_ref[...]
    step = staged.shape[0] // SPLIT
    for i in range(SPLIT):
        cells = lax.broadcasted_iota(jnp.int32, (step, cell_ref.shape[1]), 0) + i * step
        one_hot = (cells == cell_ref[...]).astype(jnp.bfloat16)
        staged[pl.ds(i * step, step)] = jnp.dot(
            one_hot, normed, preferred_element_type=jnp.float32
        ).astype(jnp.bfloat16)
        rows = pl.ds(i * step, step)
        copies.append(pltpu.make_async_copy(staged.at[rows], out_ref.at[rows], sems.at[i]))
        copies[-1].start()
    for copy in copies:
        copy.wait()


def norm_and_send(pre, attn, weights, depth, gain, cell, cells):
    tok, width = pre.shape
    weights = weights[depth:]
    whole = pl.BlockSpec(memory_space=pltpu.VMEM)
    return pl.pallas_call(
        norm_kernel,
        out_shape=[
            pltpu.HBM((tok, width), jnp.float32),
            jax.ShapeDtypeStruct((tok, width), jnp.bfloat16),
            pltpu.HBM((cells, width), jnp.bfloat16),
        ],
        grid=(1,),
        in_specs=[whole] * (1 + len(attn))
        + [whole] * 3,
        out_specs=[
            pl.BlockSpec(memory_space=pltpu.HBM),
            whole,
            pl.BlockSpec(memory_space=pltpu.HBM),
        ],
        scratch_shapes=[
            pltpu.VMEM((tok, width), jnp.float32),
            pltpu.VMEM((cells, width), jnp.bfloat16),
            pltpu.SemaphoreType.DMA((2 * SPLIT,)),
        ],
        compiler_params=pltpu.CompilerParams(vmem_limit_bytes=24 << 20),
        name="norm",
    )(pre, *attn, weights, gain[None, :], cell[None, :])


def chosen_rows(cell, back):
    cells = lax.broadcasted_iota(jnp.int32, (cell.shape[0], back.shape[0]), 1)
    one_hot = (cells == cell).astype(jnp.bfloat16)
    return jnp.dot(one_hot, back, preferred_element_type=jnp.float32)


def rows_kernel(hidden_ref, gate_ref, cell_ref, next_ref, back_ref, out_ref):
    width = hidden_ref.shape[1]
    rows = chosen_rows(cell_ref[...], back_ref[...])
    out_ref[:, :width] = hidden_ref[...] + gate_ref[...] * rows
    lane = lax.broadcasted_iota(jnp.int32, (out_ref.shape[0], SIDE), 1)
    out_ref[:, width:] = jnp.where(
        lane == 0, gate_ref[...], next_ref[...].astype(jnp.float32)
    )


def first_rows(hidden, gate, cell, next_cell, back):
    tok, width = hidden.shape
    return pl.pallas_call(
        rows_kernel,
        out_shape=jax.ShapeDtypeStruct((tok, width + SIDE), jnp.float32),
        compiler_params=pltpu.CompilerParams(vmem_limit_bytes=24 << 20),
        name="rows",
    )(hidden, gate, cell[:, None], next_cell[:, None], back)


def final_kernel(base_ref, back, out_ref, staged, sems):
    tok, width = staged.shape
    step = tok // SPLIT
    copies = []
    for i in range(SPLIT):
        rows = pl.ds(i * step, step)
        gate = base_ref[rows, width : width + 1]
        cell = base_ref[rows, width + 1 : width + 2].astype(jnp.int32)
        chosen = chosen_rows(cell, back[...])
        staged[rows] = (base_ref[rows, :width] + gate * chosen).astype(jnp.bfloat16)
        copies.append(pltpu.make_async_copy(staged.at[rows], out_ref.at[rows], sems.at[i]))
        copies[-1].start()
    for copy in copies:
        copy.wait()


def last_rows(base, back):
    shape = (base.shape[0], base.shape[1] - SIDE)
    return pl.pallas_call(
        final_kernel,
        out_shape=pltpu.HBM(shape, jnp.bfloat16),
        in_specs=[pl.BlockSpec(memory_space=pltpu.VMEM)] * 2,
        out_specs=pl.BlockSpec(memory_space=pltpu.HBM),
        scratch_shapes=[
            pltpu.VMEM(shape, jnp.bfloat16),
            pltpu.SemaphoreType.DMA((SPLIT,)),
        ],
        compiler_params=pltpu.CompilerParams(vmem_limit_bytes=16 << 20),
        name="final",
    )(base, back)


def expert_kernel(x_ref, up_ref, down_ref, o_ref, total):
    i = pl.program_id(0)
    last = pl.num_programs(0) - 1
    half = up_ref.shape[1] // 2
    part = None
    for s in range(2):
        lifted = jnp.dot(
            x_ref[...], up_ref[:, s * half : (s + 1) * half], preferred_element_type=jnp.float32
        )
        lifted = jax.nn.gelu(lifted, approximate=True).astype(jnp.bfloat16)
        down = jnp.dot(
            lifted, down_ref[s * half : (s + 1) * half, :], preferred_element_type=jnp.float32
        )
        part = down if part is None else part + down

    @pl.when(i == 0)
    def _():
        total[...] = part

    @pl.when(jnp.logical_and(i > 0, i < last))
    def _():
        total[...] += part

    @pl.when(i == last)
    def _():
        o_ref[...] = (total[...] + part).astype(jnp.bfloat16)


def run_expert(rows, up_matrix, down_matrix):
    count, hidden = rows.shape[0], up_matrix.shape[1]
    step = 1024
    return pl.pallas_call(
        expert_kernel,
        out_shape=jax.ShapeDtypeStruct((count, D), jnp.bfloat16),
        grid=(hidden // step,),
        in_specs=[
            pl.BlockSpec((count, D), lambda i: (0, 0)),
            pl.BlockSpec((D, step), lambda i: (0, i)),
            pl.BlockSpec((step, D), lambda i: (i, 0)),
        ],
        out_specs=pl.BlockSpec((count, D), lambda i: (0, 0)),
        scratch_shapes=[pltpu.VMEM((count, D), jnp.float32)],
        compiler_params=pltpu.CompilerParams(vmem_limit_bytes=58 << 20),
        cost_estimate=pl.CostEstimate(
            flops=4 * count * D * hidden, transcendentals=count * hidden, bytes_accessed=4 * D * hidden
        ),
        name="expert",
    )(rows, up_matrix, down_matrix)


def layer(
    tokens,
    queries,
    keys,
    values,
    neighbours,
    live_bits,
    out_proj,
    norm_gain,
    router,
    expert,
    slot,
    w_up,
    w_down,
):
    tok_dev = tokens.shape[0]
    tiles_dev = tok_dev // TILE
    experts = router.shape[1]
    cap = 2 * tok_dev // experts
    my_node = lax.axis_index("node")
    node_count = lax.axis_size("node")
    column_count = lax.axis_size("expert")
    swap = [(i, i ^ 1) for i in range(node_count)]
    onward = [(i, (i + 2 - 4 * (i % 2)) % node_count) for i in range(node_count)]
    is_odd = my_node % 2
    owner_node = neighbours // tiles_dev // column_count
    offset = (owner_node - my_node + node_count) % node_count
    near_offset = jnp.where(is_odd == 1, node_count - 1, 1)
    block_of = jnp.where(offset == 0, 0, jnp.where(offset == near_offset, 1, 2))
    position = block_of * (2 * tiles_dev) + neighbours % tiles_dev
    cols, col = [], 0
    for pairs in SEND_PAIRS:
        cols.append((col, pairs * PAIR))
        col += pairs * PAIR
    owns = pack(keys, values, cols[:1])
    owns += pack(keys, values, cols[1:])
    sent = []
    for i, own in enumerate(owns):
        near = lax.ppermute(own, "node", swap)
        far = lax.ppermute(near, "node", onward)
        sent.append((own, near, far))
    mixed, i, col = [], 0, 0
    for length in GROUPS:
        sizes = SEND_PAIRS[i : i + length]
        width = sum(sizes) * PAIR
        blocks = [block for chunk in sent[i : i + length] for block in chunk]
        mixed.append(attend(queries, col, sizes, blocks, position, live_bits))
        i, col = i + length, col + width
    part_cap = cap // PARTS
    slot_cell = expert * part_cap + slot % part_cap
    cells = [jnp.where(slot // part_cap == part, slot_cell, -1) for part in range(PARTS)]
    early = jnp.concatenate(mixed[:EARLY], axis=1)
    depth = early.shape[1]
    pre = tokens.astype(jnp.float32) + jnp.dot(
        early, out_proj[:depth], preferred_element_type=jnp.float32
    )
    hidden, normed, outgoing = norm_and_send(
        pre, mixed[EARLY:], out_proj, depth, norm_gain, cells[0], experts * part_cap
    )
    logits = jnp.dot(normed, router, preferred_element_type=jnp.float32)
    columns = lax.iota(jnp.int32, experts)
    chosen = jnp.sum(jnp.where(columns[None, :] == expert[:, None], logits, 0.0), axis=-1)
    gate = jax.nn.sigmoid(chosen)[:, None]
    layer_out = hidden
    for part in range(PARTS):
        if part:
            one_hot = lax.iota(jnp.int32, experts * part_cap)[:, None] == cells[part][None, :]
            outgoing = jnp.dot(
                one_hot.astype(jnp.bfloat16), normed, preferred_element_type=jnp.float32
            ).astype(jnp.bfloat16)
        block = lax.all_to_all(
            outgoing.reshape(experts, part_cap, D),
            ("node", "expert"),
            split_axis=0,
            concat_axis=0,
            tiled=True,
        )
        result = run_expert(block.reshape(-1, D), w_up[0], w_down[0])
        returned = lax.all_to_all(
            result.reshape(block.shape),
            ("node", "expert"),
            split_axis=0,
            concat_axis=0,
            tiled=True,
        )
        returned = returned.reshape(experts * part_cap, D)
        if part < PARTS - 1:
            layer_out = first_rows(layer_out, gate, cells[part], cells[part + 1], returned)
        else:
            layer_out = last_rows(layer_out, returned)
    return layer_out


def solution(mesh):
    in_specs = (
        P(("node", "expert"), None),
        P(("node", "expert"), None),
        P(("node", "expert"), None),
        P(("node", "expert"), None),
        P(("node", "expert"), None),
        P(("node", "expert"), None),
        P(),
        P(),
        P(),
        P(("node", "expert")),
        P(("node", "expert")),
        P(("node", "expert"), None, None),
        P(("node", "expert"), None, None),
    )
    out_specs = P(("node", "expert"), None)
    return jax.shard_map(layer, mesh=mesh, in_specs=in_specs, out_specs=out_specs, check_vma=False)
```
